32 devices in a mesh: vocab: 16 (over z, y, x), tok: 2 (over core).
Axes of the slice: x: 2, y: 2, z: 4, core: 2. Of those that a mesh axis runs over, the one named last changes fastest.
Arguments:
- hidden: bfloat16 [384, 3584], P('vocab', 'tok'), may hold values from -6 to 6
- embedding: bfloat16 [131072, 3584], P('vocab', 'tok'), may hold values from -0.3125 to 0.3125
- embed_cotangent: bfloat16 [384, 3584], P('vocab', 'tok'), may hold values from -0.119628906 to 0.119628906
- input_ids: int32 [384], P('vocab'), may hold values from 0 to 131071
- target_ids: int32 [384], P('vocab'), may hold values from 0 to 131071
Outputs:
- embedding_grad: bfloat16 [131072, 3584], P('vocab', 'tok')
- hidden_grad: bfloat16 [384, 3584], P('vocab', 'tok')
- token_loss: float32 [384], P('vocab')
The draws below stay inside these ranges and needn't reach their ends.
All inputs are finite; a program needn't handle non-finite values.
Results may differ from the reference program's by a relative error of at most 0.0037.
Values may be sent and summed in bfloat16 or wider, within the bound.
No kernel may reach another device: no remote copies, remote signals or barrier semaphores. Data moves between devices by JAX's collectives and lax.ppermute only.
A program may use at most 192 MiB of HBM per device.

```python
import math
import jax
import jax.numpy as jnp
import numpy as np
from jax import lax

D = 3584
VOCAB = 131072
TOKENS = 384


def touch_ends(values, rng, smallest, top_value):
    index_at = [jax.random.randint(jax.random.fold_in(rng, axis), (), 0, length) for axis, length in enumerate(values.shape)]
    main_axis = values.shape.index(max(values.shape))
    next_to = index_at[:main_axis] + [(index_at[main_axis] + 1) % values.shape[main_axis]] + index_at[main_axis + 1:]
    return values.at[tuple(index_at)].set(smallest).at[tuple(next_to)].set(top_value)


def block_levels(own_key, shape, cuts, low, high):
    def one(axis_at, blocks):
        heights = jax.random.uniform(jax.random.fold_in(jax.random.fold_in(own_key, 6), axis_at), (blocks,), jnp.float32, low / len(cuts), high / len(cuts))
        return jnp.repeat(jnp.exp(heights), shape[axis_at] // blocks).reshape((-1,) + (1,) * (len(shape) - axis_at - 1))

    loudness = one(*cuts[0])
    for cut in cuts[1:]:
        loudness = loudness * one(*cut)
    return loudness


def skewed_wide(own_key, extent, count, slope):
    loads = [min(1 << octave, count + 1 - (1 << octave)) * (1 << 20) // math.isqrt((1 << octave) ** slope) + 1 for octave in range((count + 1).bit_length()) if 1 << octave <= count]
    deviation = 1 + sum(loads) // (1 << 30)
    table = np.cumsum(np.array([max(1, weight // deviation) for weight in loads]))
    pick = jax.random.randint(jax.random.fold_in(own_key, 1), extent, 0, int(table[len(loads) - 1]))
    start = jnp.left_shift(1, jnp.searchsorted(jnp.asarray(table, jnp.int32), pick, side="right").astype(jnp.int32))
    grade = start - 1 + jax.random.randint(jax.random.fold_in(own_key, 4), extent, 0, 1 << 30) % jnp.minimum(start, count + 1 - start)
    return jax.random.permutation(jax.random.fold_in(own_key, 2), count)[grade].astype(jnp.int32)


def normal_values(own_key, dims, deviation, reach, split=(), kind=jnp.bfloat16):
    array = deviation * jax.random.normal(own_key, dims, jnp.float32)
    if split:
        array = array * block_levels(own_key, dims, split, -0.22, 0.18)
    return jnp.clip(array, -reach, reach).astype(kind)


def setup_inputs(seed: int = 0) -> dict:
    arg_keys = jax.random.split(jax.random.key(seed), 6)
    hidden = normal_values(arg_keys[0], (TOKENS, D), 1.0, 6.0, ((0, 16), (1, 2)))
    embedding = normal_values(arg_keys[1], (VOCAB, D), (D // 9) ** -0.5, 0.3125, ((0, 16), (1, 2)))
    embed_cotangent = normal_values(arg_keys[2], (TOKENS, D), 0.02, 0.119628906, ((0, 16), (1, 2)))
    input_ids = touch_ends(skewed_wide(arg_keys[3], (TOKENS,), VOCAB, 2), jax.random.fold_in(arg_keys[3], 3), 0, VOCAB - 1).astype(jnp.int32)
    target_ids = touch_ends(skewed_wide(arg_keys[4], (TOKENS,), VOCAB, 2), jax.random.fold_in(arg_keys[4], 3), 0, VOCAB - 1).astype(jnp.int32)
    return {"hidden": hidden, "embedding": embedding, "embed_cotangent": embed_cotangent, "input_ids": input_ids, "target_ids": target_ids}


softcap = 30.0
zloss_weight = 0.001

def reference(hidden, embedding, embed_cotangent, input_ids, target_ids):
    raw_logits = jnp.dot(hidden, embedding.T, preferred_element_type=jnp.float32)
    capped = softcap * jnp.tanh(raw_logits / softcap)
    exponent = jnp.exp(capped - softcap)
    row_total = lax.optimization_barrier(jnp.sum(exponent, axis=1))
    log_total = softcap + jnp.log(row_total)
    vocab_pos = jnp.arange(VOCAB, dtype=jnp.int32)
    target_hot = target_ids[:, None] == vocab_pos[None, :]
    target_logit = lax.optimization_barrier(jnp.sum(jnp.where(target_hot, capped, jnp.zeros_like(capped)), axis=1))
    token_loss = log_total - target_logit + zloss_weight * log_total * log_total
    factor = 1.0 + 2.0 * zloss_weight * log_total
    capped_grad = factor[:, None] * exponent / row_total[:, None] - target_hot.astype(jnp.float32)
    ratio = capped / softcap
    logit_grad = (capped_grad * (1.0 - ratio * ratio)).astype(jnp.bfloat16)
    hidden_grad = jnp.dot(logit_grad, embedding, preferred_element_type=jnp.float32).astype(jnp.bfloat16)
    input_hot = (input_ids[:, None] == vocab_pos[None, :]).astype(jnp.bfloat16)
    embed_scale = math.sqrt(D)
    block_count = math.gcd(VOCAB, 32)
    grad_blocks = logit_grad.T.reshape(block_count, VOCAB // block_count, TOKENS)
    hot_blocks = input_hot.T.reshape(block_count, VOCAB // block_count, TOKENS)

    def one_block(pair):
        grad_rows, hot_rows = pair
        head_grad = jnp.dot(grad_rows, hidden, preferred_element_type=jnp.float32)
        inject = jnp.dot(hot_rows, embed_cotangent, preferred_element_type=jnp.float32)
        return (head_grad + embed_scale * inject).astype(jnp.bfloat16)
    embedding_grad = lax.map(one_block, (grad_blocks, hot_blocks)).reshape(VOCAB, D)
    return (embedding_grad, hidden_grad, token_loss)
```

```python
import functools
import math

import jax
import jax.numpy as jnp
from jax import lax
from jax.experimental import pallas as pl
from jax.experimental.pallas import tpu as pltpu
from jax.sharding import PartitionSpec as P


softcap = 30.0
zloss_weight = 0.001
f32 = jnp.float32
bf16 = jnp.bfloat16


def column_stats(logits, first_column, targets):
    capped = softcap * jnp.tanh(logits / softcap)
    exponent = jnp.exp(capped - softcap)
    columns = first_column + jnp.arange(logits.shape[1], dtype=jnp.int32)
    target_hot = targets[:, None] == columns[None, :]
    local_total = jnp.sum(exponent, axis=1)
    local_target = jnp.sum(jnp.where(target_hot, capped, jnp.zeros_like(capped)), axis=1)
    return (capped, exponent, target_hot, local_total, local_target)


def column_grad(capped, exponent, target_hot, row_total, log_total):
    factor = 1.0 + 2.0 * zloss_weight * log_total
    capped_grad = factor[:, None] * exponent / row_total[:, None] - target_hot.astype(f32)
    ratio = capped / softcap
    return (capped_grad * (1.0 - ratio * ratio)).astype(bf16)


def plain(hidden, embedding, embed_cotangent, input_ids, target_ids, tok_count):
    gather = functools.partial(lax.all_gather, axis_name="vocab", axis=0, tiled=True)
    gathered, cotangent = gather(hidden), gather(embed_cotangent)
    input_all, target_all = gather(input_ids), gather(target_ids)
    rows_here = embedding.shape[0]
    partial_value = lax.dot_general(gathered, embedding, (((1,), (1,)), ((), ())), preferred_element_type=f32)
    first_row = lax.axis_index("vocab") * rows_here
    logits = lax.psum(partial_value, "tok")
    capped, exponent, target_hot, local_total, local_target = column_stats(logits, first_row, target_all)
    row_total, target_logit = lax.psum((local_total, local_target), "vocab")
    log_total = softcap + jnp.log(row_total)
    logit_grad = column_grad(capped, exponent, target_hot, row_total, log_total)
    loss_all = log_total - target_logit + zloss_weight * log_total * log_total
    local_count = input_ids.shape[0]
    token_loss = lax.dynamic_slice_in_dim(loss_all, lax.axis_index("vocab") * local_count, local_count, 0)
    hidden_grad = lax.psum_scatter(
        jnp.dot(logit_grad, embedding, preferred_element_type=f32), "vocab", scatter_dimension=0, tiled=True
    ).astype(bf16)
    columns = first_row + jnp.arange(rows_here, dtype=jnp.int32)
    input_hot = (input_all[:, None] == columns[None, :]).astype(bf16)
    head_grad = lax.dot_general(logit_grad, gathered, (((0,), (0,)), ((), ())), preferred_element_type=f32)
    inject = lax.dot_general(input_hot, cotangent, (((0,), (0,)), ((), ())), preferred_element_type=f32)
    embed_scale = math.sqrt(hidden.shape[1] * tok_count)
    embedding_grad = (head_grad + embed_scale * inject).astype(bf16)
    return (embedding_grad, hidden_grad, token_loss)


def dot(a, b, ca, cb):
    return lax.dot_general(a, b, (((ca,), (cb,)), ((), ())), preferred_element_type=f32)


def params(*names, vmem=None):
    return pltpu.CompilerParams(dimension_semantics=names, vmem_limit_bytes=vmem)


def cost(flops, nbytes, trans=0):
    return pl.CostEstimate(flops=flops, bytes_accessed=nbytes, transcendentals=trans)


def swap(x, bit, count):
    return lax.ppermute(x, "vocab", [(s, s ^ bit) for s in range(count)])


def swap_tok(x):
    return lax.ppermute(x, "tok", [(0, 1), (1, 0)])


def digits(ids):
    return [((ids >> shift) & 255).astype(bf16) for shift in (0, 8, 16)]


def undigits(columns):
    low, middle, high = (columns[:, k : k + 1].astype(f32).astype(jnp.int32) for k in range(3))
    return low + 256 * middle + 65536 * high


def side(base, far):
    return 1 - base[0] if far else base[0]


def tie(x, *others):
    return lax.optimization_barrier((x, *others))[0]


def merge_into(a0, a1, b0, b1, hid, half):
    quarter = a0.shape[0] // 2
    hid[: 2 * quarter, :half] = a0[:, :half]
    hid[2 * quarter :, :half] = a1[:, :half]
    hid[:quarter, half:] = b0[:quarter, :]
    hid[quarter : 2 * quarter, half:] = b1[:quarter, :]
    hid[2 * quarter : 3 * quarter, half:] = b0[quarter:, :]
    hid[3 * quarter :, half:] = b1[quarter:, :]


def first_kernel(base, a0, a1, b0, b1, emb, out, hid, target, inputs, *, half):
    @pl.when(pl.program_id(0) == 0)
    def _():
        merge_into(a0, a1, b0, b1, hid, half)
        size = a0.shape[0]
        for k, part in enumerate((a0, a1)):
            codes = part[:, half : half + 128]
            target[k * size : (k + 1) * size, :] = undigits(codes[:, 0:3])
            inputs[k * size : (k + 1) * size, :] = undigits(codes[:, 3:6])

    out[...] = dot(hid[...], emb[...], 1, 1)


def first_logits(base, pieces, embedding, count, block):
    _, width = embedding.shape
    tokens = 2 * pieces[0].shape[0]
    whole = lambda i, b: (0, 0)
    return pl.pallas_call(
        functools.partial(first_kernel, half=width // 2),
        grid_spec=pltpu.PrefetchScalarGridSpec(
            num_scalar_prefetch=1,
            grid=(count // block,),
            in_specs=[pl.BlockSpec(p.shape, whole) for p in pieces]
            + [pl.BlockSpec((block, width), lambda i, b: (side(b, True) * (count // block) + i, 0))],
            out_specs=[
                pl.BlockSpec((tokens, block), lambda i, b: (0, i)),
                pl.BlockSpec((tokens, width), whole),
                pl.BlockSpec((tokens, 1), whole),
                pl.BlockSpec((tokens, 1), whole),
            ],
        ),
        out_shape=[
            jax.ShapeDtypeStruct((tokens, count), f32),
            jax.ShapeDtypeStruct((tokens, width), bf16),
            jax.ShapeDtypeStruct((tokens, 1), jnp.int32),
            jax.ShapeDtypeStruct((tokens, 1), jnp.int32),
        ],
        compiler_params=params("arbitrary"),
        cost_estimate=cost(2 * tokens * width * count, 2 * width * count),
    )(base, *pieces, embedding)


def logits_kernel(base, hid, emb, other, target, bent_ref, stats_ref, total, picked, slope, *, block, rows):
    step = pl.program_id(0)

    @pl.when(step == 0)
    def _():
        total[...] = jnp.zeros_like(total)
        picked[...] = jnp.zeros_like(picked)
        slope[...] = jnp.zeros_like(slope)

    logits = dot(hid[...], emb[...], 1, 1) + other[...]
    ratio = jnp.tanh(logits * (1.0 / softcap))
    exponent = jnp.exp(softcap * ratio - softcap)
    here = target[...] - (base[1] * rows + base[0] * (rows // 2) + step * block)
    lane = lax.broadcasted_iota(jnp.int32, ratio.shape, 1)
    chosen = jnp.where(lane == here, ratio, 0.0)
    bent = exponent * (1.0 - ratio * ratio)
    bent_ref[...] = bent
    total[...] += sum(exponent[:, k : k + 128] for k in range(0, block, 128))
    picked[...] += sum(chosen[:, k : k + 128] for k in range(0, block, 128))
    slope[...] += sum(bent[:, k : k + 128] for k in range(0, block, 128))

    @pl.when(step == pl.num_programs(0) - 1)
    def _():
        stats_ref[...] = jnp.zeros_like(stats_ref)
        stats_ref[0:1, :] = jnp.sum(total[...].T, axis=0, keepdims=True)
        stats_ref[1:2, :] = jnp.sum(picked[...].T, axis=0, keepdims=True)
        stats_ref[2:3, :] = jnp.sum(slope[...].T, axis=0, keepdims=True)


def own_logits(base, hid, embedding, other, target, block):
    tokens, width = hid.shape
    count = other.shape[1]
    return pl.pallas_call(
        functools.partial(logits_kernel, block=block, rows=embedding.shape[0]),
        grid_spec=pltpu.PrefetchScalarGridSpec(
            num_scalar_prefetch=1,
            grid=(count // block,),
            in_specs=[
                pl.BlockSpec((tokens, width), lambda i, b: (0, 0)),
                pl.BlockSpec((block, width), lambda i, b: (b[0] * (count // block) + i, 0)),
                pl.BlockSpec((tokens, block), lambda i, b: (0, i)),
                pl.BlockSpec((tokens, 1), lambda i, b: (0, 0)),
            ],
            out_specs=[
                pl.BlockSpec((tokens, block), lambda i, b: (0, i)),
                pl.BlockSpec((8, tokens), lambda i, b: (0, 0)),
            ],
            scratch_shapes=[pltpu.VMEM((tokens, 128), f32) for _ in range(3)],
        ),
        out_shape=[jax.ShapeDtypeStruct((tokens, count), f32), jax.ShapeDtypeStruct((8, tokens), f32)],
        compiler_params=params("arbitrary"),
        cost_estimate=cost(2 * tokens * width * count, 2 * width * count),
    )(base, hid, embedding, other, target)


def hidden_kernel(base, near, far, emb, stats_ref, target, grad_ref, *rest, block, tiles, rows):
    left_keep, left_sent, right_keep, right_sent, total, column = rest
    step = pl.program_id(0)

    @pl.when(step == 0)
    def _():
        total[...] = jnp.zeros_like(total)
        stats = stats_ref[...].T
        row_total, ratio, slope = stats[:, 0:1], stats[:, 1:2], stats[:, 2:3]
        column[0] = (1.0 + 2.0 * zloss_weight * (softcap + jnp.log(row_total))) / row_total
        column[1] = 1.0 - ratio * ratio
        column[2] = 1.0 / sent_scale(row_total, ratio, slope)

    first = place_of(base, step, tiles) * block + base[1] * rows

    def add(bent):
        lane = lax.broadcasted_iota(jnp.int32, bent.shape, 1)
        hot = jnp.where(lane == target[...] - first, column[1], 0.0)
        grad = (column[0] * bent[...] - hot).astype(bf16)
        grad_ref[...] = grad
        total[...] += dot(grad, emb[...], 1, 0)

    pl.when(step < tiles)(lambda: add(near))
    pl.when(step >= tiles)(lambda: add(far))

    @pl.when(step == pl.num_programs(0) - 1)
    def _():
        inverse = column[2]
        half = left_keep.shape[1]
        quarter = left_keep.shape[0] // 2
        rows_of = [slice(k * quarter, (k + 1) * quarter) for k in range(4)]
        one, two = rows_of[:2]
        left, right = slice(0, half), slice(half, 2 * half)
        for ref, at, source, columns in (
            (left_keep, one, rows_of[0], left),
            (left_keep, two, rows_of[1], left),
            (left_sent, one, rows_of[2], left),
            (left_sent, two, rows_of[3], left),
            (right_keep, one, rows_of[0], right),
            (right_keep, two, rows_of[2], right),
            (right_sent, one, rows_of[1], right),
            (right_sent, two, rows_of[3], right),
        ):
            ref[at, :] = (total[source, columns] * inverse[source, :]).astype(ref.dtype)


def place_of(base, step, tiles):
    return jnp.where(step < tiles, base[0] * tiles + step, (1 - base[0]) * tiles + step - tiles)


def sent_scale(row_total, ratio, slope):
    weight = (1.0 + 2.0 * zloss_weight * (softcap + jnp.log(row_total))) / row_total
    return jnp.maximum(weight * slope + (1.0 - ratio * ratio), 1e-30) * (1.0 / 4096.0)


def hidden_sum(base, near, far, embedding, stats, target, block):
    tokens, count = near.shape
    rows, width = embedding.shape
    tiles = count // block
    shape = (tokens // 2, width // 2)
    whole = lambda i, b: (0, 0)
    return pl.pallas_call(
        functools.partial(hidden_kernel, block=block, tiles=tiles, rows=rows),
        grid_spec=pltpu.PrefetchScalarGridSpec(
            num_scalar_prefetch=1,
            grid=(2 * tiles,),
            in_specs=[
                pl.BlockSpec((tokens, block), lambda i, b: (0, jnp.minimum(i, tiles - 1))),
                pl.BlockSpec((tokens, block), lambda i, b: (0, jnp.maximum(i - tiles, 0))),
                pl.BlockSpec((block, width), lambda i, b: (place_of(b, i, tiles), 0)),
                pl.BlockSpec((8, tokens), whole),
                pl.BlockSpec((tokens, 1), whole),
            ],
            out_specs=[pl.BlockSpec((tokens, block), lambda i, b: (0, i))] + [pl.BlockSpec(shape, whole) for _ in range(4)],
            scratch_shapes=[pltpu.VMEM((tokens, width), f32), pltpu.VMEM((3, tokens, 1), f32)],
        ),
        out_shape=[jax.ShapeDtypeStruct((tokens, rows), bf16)] + [jax.ShapeDtypeStruct(shape, f32) for _ in range(4)],
        compiler_params=params("arbitrary"),
        cost_estimate=cost(2 * tokens * width * rows, 2 * width * rows),
    )(base, near, far, embedding, stats, target)


GROUP = 16


def embed_kernel(base, listed, bounds, grad, hid, cot_a, cot_b, ids, listed_col, *rest, block, scale, skip, tiles):
    out, mixed = rest[-2:]
    out[...] = dot(grad[...], hid[...], 0, 0).astype(bf16)
    tile = place_of(base, skip + pl.program_id(0), tiles)
    split = cot_a.shape[0]
    first, last = bounds[tile], bounds[tile + 1]

    def group(g, carry):
        at = first + g * GROUP
        hot = jnp.where(listed_col[pl.ds(at, GROUP), :] == ids[...], 1.0, 0.0).astype(bf16)
        mixed[...] = scale * (dot(hot[:, :split], cot_a[...], 1, 0) + dot(hot[:, split:], cot_b[...], 1, 0))

        def one(k, carry):
            row = listed[at + k] - tile * block
            start = pl.multiple_of((row // 16) * 16, 16)
            near_row = lax.broadcasted_iota(jnp.int32, (16, out.shape[1]), 0) == row - start
            add = jnp.where(near_row, mixed[pl.ds(k, 1), :], 0.0)
            out[pl.ds(start, 16), :] = (out[pl.ds(start, 16), :].astype(f32) + add).astype(bf16)
            return carry

        return lax.fori_loop(0, jnp.minimum(GROUP, last - at), one, carry)

    lax.fori_loop(0, (last - first + GROUP - 1) // GROUP, group, 0)


def embed_grad(base, listed, bounds, grad, skip, steps, hid, cot, ids, block, scale, start):
    tokens, width = hid.shape
    rows = grad.shape[1]
    tiles = rows // block // 2
    whole = lambda i, *s: (0, 0)
    column = listed[:, None]
    extra = [] if start is None else [start]
    return pl.pallas_call(
        functools.partial(embed_kernel, block=block, scale=scale, skip=skip, tiles=tiles),
        grid_spec=pltpu.PrefetchScalarGridSpec(
            num_scalar_prefetch=3,
            grid=(steps,),
            in_specs=[
                pl.BlockSpec((tokens, block), lambda i, *s: (0, skip + i)),
                pl.BlockSpec((tokens, width), whole),
                pl.BlockSpec((tokens // 2, width), whole),
                pl.BlockSpec((tokens // 2, width), whole),
                pl.BlockSpec((1, tokens), whole),
                pl.BlockSpec(column.shape, whole),
            ]
            + [pl.BlockSpec(memory_space=pl.ANY) for _ in extra],
            out_specs=pl.BlockSpec((block, width), lambda i, b, *s: (place_of(b, skip + i, tiles), 0)),
            scratch_shapes=[pltpu.VMEM((GROUP, width), f32)],
        ),
        out_shape=jax.ShapeDtypeStruct((rows, width), bf16),
        input_output_aliases={9: 0} if extra else {},
        compiler_params=params("arbitrary"),
        cost_estimate=cost(2 * tokens * width * block * steps, 2 * width * block * steps),
    )(base, listed, bounds, grad, hid, *cot, ids, column, *extra)


def flipped(x, span):
    lane = jnp.arange(x.shape[1], dtype=jnp.int32)
    return jnp.where((lane // span) % 2 == 0, jnp.roll(x, -span, 1), jnp.roll(x, span, 1))


def local_rows(ids, first_row, rows, block):
    at = ids - first_row
    count = at.shape[0]
    order = jnp.arange(count, dtype=jnp.int32)
    repeat = jnp.any((at[:, None] == at[None, :]) & (order[None, :] < order[:, None]), axis=1)
    lead = (at >= 0) & (at < rows) & ~repeat
    rank = jnp.sum((lead[None, :] & (at[None, :] < at[:, None])).astype(jnp.int32), axis=1)
    slots = jnp.arange(count + GROUP, dtype=jnp.int32)
    listed = jnp.sum(jnp.where(lead[None, :] & (rank[None, :] == slots[:, None]), at[None, :] + 1, 0), axis=1) - 1
    edges = block * jnp.arange(rows // block + 1, dtype=jnp.int32)
    bounds = jnp.sum((lead[None, :] & (at[None, :] < edges[:, None])).astype(jnp.int32), axis=1)
    return at, listed, bounds


def permuted(hidden, embedding, embed_cotangent, input_ids, target_ids, tok_count, vocab_count):
    rows, width = embedding.shape
    own_tokens = hidden.shape[0]
    tokens = own_tokens * vocab_count
    half, half_rows = width // 2, rows // 2
    block = 1024
    bits = [vocab_count >> (k + 1) for k in range(vocab_count.bit_length() - 1)]
    core, place = lax.axis_index("tok"), lax.axis_index("vocab")
    base = jnp.stack([core, place]).astype(jnp.int32)
    across = functools.partial(swap, count=vocab_count)

    def grow(x, bit):
        return jnp.concatenate([x, across(x, bit)], axis=0)

    coded = jnp.stack(digits(target_ids) + digits(input_ids), axis=1)
    coded = jnp.pad(coded, ((0, 0), (0, 128 - coded.shape[1])))
    value = jnp.concatenate([hidden[:, :half], coded, hidden[:, half:]], axis=1)
    for bit in bits[:-2]:
        value = grow(value, bit)
    left = grow(value[:, : half + 128], bits[-2])
    right = grow(value[:, half + 128 :], bits[-1])
    left_other = across(left, bits[-1])
    right_other = across(right, bits[-2])

    cot = embed_cotangent
    for bit in bits[:-1]:
        other = across(cot, bit)
        cot = jnp.concatenate([cot, other], axis=0)

    sent, hid, target, inputs = first_logits(base, (left, left_other, right, right_other), embedding, half_rows, block)
    got = swap_tok(sent)
    input_row, listed, bounds = local_rows(inputs[:, 0], place * rows, rows, block)
    target = tie(target, listed, bounds, input_row)
    near, stats = own_logits(base, hid, embedding, got, target, block)
    far = swap_tok(near)

    stats = stats + swap_tok(stats)
    for k, bit in enumerate(bits):
        other = across(stats, bit)
        stats = stats + flipped(other, own_tokens << k)
    own_log = softcap + jnp.log(stats[0, :own_tokens])
    token_loss = own_log - softcap * stats[1, :own_tokens] + zloss_weight * own_log * own_log
    cot = (cot, across(tie(cot, stats), bits[-1]))

    grad, left, left_sent, right, right_sent = hidden_sum(base, near, far, embedding, stats, target, block)

    def fold(keep, sent, bit):
        return keep + across(sent.astype(jnp.float16), bit).astype(f32)

    embed = functools.partial(
        embed_grad, hid=hid, cot=cot, ids=input_row[None, :], block=block, scale=math.sqrt(width * tok_count)
    )
    tiles = half_rows // block
    embedding_grad = embed(base, listed, bounds, grad, 0, tiles, start=None)
    left = fold(left, left_sent, bits[-1])
    right = fold(right, right_sent, bits[-2])
    embedding_grad = embed(base, listed, bounds, grad, tiles, tiles // 2, start=embedding_grad)
    size = tokens // 4
    left = fold(left[:size], left[size:], bits[-2])
    right = fold(right[:size], right[size:], bits[-1])
    embedding_grad = embed(
        base, listed, bounds, grad, tiles + tiles // 2, tiles - tiles // 2, start=embedding_grad
    )
    value = jnp.concatenate([left, right], axis=1)
    blocks = [value[k * own_tokens : (k + 1) * own_tokens] for k in range(4)]
    hidden_grad = blocks[0]
    for block_, bit in zip(blocks[1:], (bits[0], bits[1], bits[0] ^ bits[1])):
        hidden_grad = fold(hidden_grad, block_, bit)
    own = stats[:, :own_tokens]
    hidden_grad = (hidden_grad * sent_scale(own[0], own[1], own[2])[:, None]).astype(bf16)
    return (embedding_grad, hidden_grad, token_loss)


def solution(mesh):
    vocab_count, tok_count = mesh.shape["vocab"], mesh.shape["tok"]
    paired = tok_count == 2 and vocab_count == 16

    def local(hidden, embedding, embed_cotangent, input_ids, target_ids):
        rows, width = embedding.shape
        args = (hidden, embedding, embed_cotangent, input_ids, target_ids, tok_count)
        if not paired:
            return plain(*args)
        assert rows % 2048 == 0 and width % 256 == 0
        return permuted(*args, vocab_count)

    return jax.shard_map(
        local,
        mesh=mesh,
        in_specs=(P("vocab", "tok"), P("vocab", "tok"), P("vocab", "tok"), P("vocab"), P("vocab")),
        out_specs=(P("vocab", "tok"), P("vocab", "tok"), P("vocab")),
        check_vma=False,
    )
```

```python
import functools
import math

import jax
import jax.numpy as jnp
from jax import lax
from jax.experimental import pallas as pl
from jax.experimental.pallas import tpu as pltpu
from jax.sharding import PartitionSpec as P


softcap = 30.0
zloss_weight = 0.001
f32 = jnp.float32
bf16 = jnp.bfloat16
f16 = jnp.float16


def column_stats(logits, first_column, targets):
    capped = softcap * jnp.tanh(logits / softcap)
    exponent = jnp.exp(capped - softcap)
    columns = first_column + jnp.arange(logits.shape[1], dtype=jnp.int32)
    target_hot = targets[:, None] == columns[None, :]
    local_total = jnp.sum(exponent, axis=1)
    local_target = jnp.sum(jnp.where(target_hot, capped, jnp.zeros_like(capped)), axis=1)
    return (capped, exponent, target_hot, local_total, local_target)


def column_grad(capped, exponent, target_hot, row_total, log_total):
    factor = 1.0 + 2.0 * zloss_weight * log_total
    capped_grad = factor[:, None] * exponent / row_total[:, None] - target_hot.astype(f32)
    ratio = capped / softcap
    return (capped_grad * (1.0 - ratio * ratio)).astype(bf16)


def plain(hidden, embedding, embed_cotangent, input_ids, target_ids, tok_count):
    gather = functools.partial(lax.all_gather, axis_name="vocab", axis=0, tiled=True)
    gathered, cotangent = gather(hidden), gather(embed_cotangent)
    input_all, target_all = gather(input_ids), gather(target_ids)
    rows_here = embedding.shape[0]
    partial_value = lax.dot_general(gathered, embedding, (((1,), (1,)), ((), ())), preferred_element_type=f32)
    first_row = lax.axis_index("vocab") * rows_here
    logits = lax.psum(partial_value, "tok")
    capped, exponent, target_hot, local_total, local_target = column_stats(logits, first_row, target_all)
    row_total, target_logit = lax.psum((local_total, local_target), "vocab")
    log_total = softcap + jnp.log(row_total)
    logit_grad = column_grad(capped, exponent, target_hot, row_total, log_total)
    loss_all = log_total - target_logit + zloss_weight * log_total * log_total
    local_count = input_ids.shape[0]
    token_loss = lax.dynamic_slice_in_dim(loss_all, lax.axis_index("vocab") * local_count, local_count, 0)
    hidden_grad = lax.psum_scatter(
        jnp.dot(logit_grad, embedding, preferred_element_type=f32), "vocab", scatter_dimension=0, tiled=True
    ).astype(bf16)
    columns = first_row + jnp.arange(rows_here, dtype=jnp.int32)
    input_hot = (input_all[:, None] == columns[None, :]).astype(bf16)
    head_grad = lax.dot_general(logit_grad, gathered, (((0,), (0,)), ((), ())), preferred_element_type=f32)
    inject = lax.dot_general(input_hot, cotangent, (((0,), (0,)), ((), ())), preferred_element_type=f32)
    embed_scale = math.sqrt(hidden.shape[1] * tok_count)
    embedding_grad = (head_grad + embed_scale * inject).astype(bf16)
    return (embedding_grad, hidden_grad, token_loss)


def dot(a, b, ca, cb):
    return lax.dot_general(a, b, (((ca,), (cb,)), ((), ())), preferred_element_type=f32)


def params(mebibytes):
    return pltpu.CompilerParams(dimension_semantics=("arbitrary",), vmem_limit_bytes=mebibytes << 20)


def cost(flops, nbytes, trans=0):
    return pl.CostEstimate(flops=flops, bytes_accessed=nbytes, transcendentals=trans)


def swap(x, bit, count):
    return lax.ppermute(x, "vocab", [(s, s ^ bit) for s in range(count)])


def swap_tok(x):
    return lax.ppermute(x, "tok", [(0, 1), (1, 0)])


def digits(ids):
    return [((ids >> shift) & 255).astype(bf16) for shift in (0, 8, 16)]


def undigits(columns):
    low, middle, high = (columns[:, k : k + 1].astype(f32).astype(jnp.int32) for k in range(3))
    return low + 256 * middle + 65536 * high


def side(base, far):
    return 1 - base[0] if far else base[0]


def tie(x, *others):
    return lax.optimization_barrier((x, *others))[0]


def merge_into(a0, a1, b0, b1, hid, half):
    quarter = a0.shape[0] // 2
    hid[: 2 * quarter, :half] = a0[:, :half]
    hid[2 * quarter :, :half] = a1[:, :half]
    hid[:quarter, half:] = b0[:quarter, :]
    hid[quarter : 2 * quarter, half:] = b1[:quarter, :]
    hid[2 * quarter : 3 * quarter, half:] = b0[quarter:, :]
    hid[3 * quarter :, half:] = b1[quarter:, :]


def first_kernel(base, a0, a1, b0, b1, emb, out, hid, target, inputs, *, half):
    @pl.when(pl.program_id(0) == 0)
    def _():
        merge_into(a0, a1, b0, b1, hid, half)
        size = a0.shape[0]
        for k, part in enumerate((a0, a1)):
            codes = part[:, half : half + 128]
            target[k * size : (k + 1) * size, :] = undigits(codes[:, 0:3])
            inputs[k * size : (k + 1) * size, :] = undigits(codes[:, 3:6])

    out[...] = dot(hid[...], emb[...], 1, 1)


def first_logits(base, pieces, embedding, count, block):
    _, width = embedding.shape
    tokens = 2 * pieces[0].shape[0]
    whole = lambda i, b: (0, 0)
    return pl.pallas_call(
        functools.partial(first_kernel, half=width // 2),
        grid_spec=pltpu.PrefetchScalarGridSpec(
            num_scalar_prefetch=1,
            grid=(count // block,),
            in_specs=[pl.BlockSpec(p.shape, whole) for p in pieces]
            + [pl.BlockSpec((block, width), lambda i, b: (side(b, True) * (count // block) + i, 0))],
            out_specs=[
                pl.BlockSpec((tokens, block), lambda i, b: (0, i)),
                pl.BlockSpec((tokens, width), whole),
                pl.BlockSpec((tokens, 1), whole),
                pl.BlockSpec((tokens, 1), whole),
            ],
        ),
        out_shape=[
            jax.ShapeDtypeStruct((tokens, count), f32),
            jax.ShapeDtypeStruct((tokens, width), bf16),
            jax.ShapeDtypeStruct((tokens, 1), jnp.int32),
            jax.ShapeDtypeStruct((tokens, 1), jnp.int32),
        ],
        compiler_params=params(28),
        cost_estimate=cost(2 * tokens * width * count, 2 * width * count),
    )(base, *pieces, embedding)


def logits_kernel(base, hid, emb, other, target, bent_ref, stats_ref, total, picked, slope, *, block, rows):
    step = pl.program_id(0)

    @pl.when(step == 0)
    def _():
        total[...] = jnp.zeros_like(total)
        picked[...] = jnp.zeros_like(picked)
        slope[...] = jnp.zeros_like(slope)

    logits = dot(hid[...], emb[...], 1, 1) + other[...]
    ratio = jnp.tanh(logits * (1.0 / softcap))
    exponent = jnp.exp(softcap * ratio - softcap)
    here = target[...] - (base[1] * rows + base[0] * (rows // 2) + step * block)
    lane = lax.broadcasted_iota(jnp.int32, ratio.shape, 1)
    chosen = jnp.where(lane == here, ratio, 0.0)
    bent = exponent * (1.0 - ratio * ratio)
    bent_ref[...] = bent
    total[...] += sum(exponent[:, k : k + 128] for k in range(0, block, 128))
    picked[...] += sum(chosen[:, k : k + 128] for k in range(0, block, 128))
    slope[...] += sum(bent[:, k : k + 128] for k in range(0, block, 128))

    @pl.when(step == pl.num_programs(0) - 1)
    def _():
        stats_ref[...] = jnp.zeros_like(stats_ref)
        stats_ref[0:1, :] = jnp.sum(total[...].T, axis=0, keepdims=True)
        stats_ref[1:2, :] = jnp.sum(picked[...].T, axis=0, keepdims=True)
        stats_ref[2:3, :] = jnp.sum(slope[...].T, axis=0, keepdims=True)


def own_logits(base, hid, embedding, other, target, block):
    tokens, width = hid.shape
    count = other.shape[1]
    return pl.pallas_call(
        functools.partial(logits_kernel, block=block, rows=embedding.shape[0]),
        grid_spec=pltpu.PrefetchScalarGridSpec(
            num_scalar_prefetch=1,
            grid=(count // block,),
            in_specs=[
                pl.BlockSpec((tokens, width), lambda i, b: (0, 0)),
                pl.BlockSpec((block, width), lambda i, b: (b[0] * (count // block) + i, 0)),
                pl.BlockSpec((tokens, block), lambda i, b: (0, i)),
                pl.BlockSpec((tokens, 1), lambda i, b: (0, 0)),
            ],
            out_specs=[
                pl.BlockSpec((tokens, block), lambda i, b: (0, i)),
                pl.BlockSpec((8, tokens), lambda i, b: (0, 0)),
            ],
            scratch_shapes=[pltpu.VMEM((tokens, 128), f32) for _ in range(3)],
        ),
        out_shape=[jax.ShapeDtypeStruct((tokens, count), f32), jax.ShapeDtypeStruct((8, tokens), f32)],
        compiler_params=params(30),
        cost_estimate=cost(2 * tokens * width * count, 2 * width * count),
    )(base, hid, embedding, other, target)


def hidden_kernel(base, near, far, emb, stats_ref, target, grad_ref, *rest, block, tiles, rows):
    keep, sent, total, column = rest
    step = pl.program_id(0)

    @pl.when(step == 0)
    def _():
        total[...] = jnp.zeros_like(total)
        stats = stats_ref[...].T
        row_total, ratio, slope = stats[:, 0:1], stats[:, 1:2], stats[:, 2:3]
        column[0] = (1.0 + 2.0 * zloss_weight * (softcap + jnp.log(row_total))) / row_total
        column[1] = 1.0 - ratio * ratio
        column[2] = 1.0 / sent_scale(row_total, ratio, slope)

    first = place_of(base, step, tiles) * block + base[1] * rows

    def add(bent):
        lane = lax.broadcasted_iota(jnp.int32, bent.shape, 1)
        hot = jnp.where(lane == target[...] - first, column[1], 0.0)
        grad = (column[0] * bent[...] - hot).astype(bf16)
        grad_ref[...] = grad
        total[...] += dot(grad, emb[...], 1, 0)

    pl.when(step < tiles)(lambda: add(near))
    pl.when(step >= tiles)(lambda: add(far))

    @pl.when(step == pl.num_programs(0) - 1)
    def _():
        size = keep.shape[0]
        keep[...] = total[:size, :] * column[2][:size]
        sent[...] = total[size:, :] * column[2][size:]


def place_of(base, step, tiles):
    return jnp.where(step < tiles, base[0] * tiles + step, (1 - base[0]) * tiles + step - tiles)


def sent_scale(row_total, ratio, slope):
    weight = (1.0 + 2.0 * zloss_weight * (softcap + jnp.log(row_total))) / row_total
    return jnp.maximum(weight * slope + (1.0 - ratio * ratio), 1e-30) * (1.0 / 4096.0)


def hidden_sum(base, near, far, embedding, stats, target, block):
    tokens, count = near.shape
    rows, width = embedding.shape
    tiles = count // block
    shape = (tokens // 2, width)
    whole = lambda i, b: (0, 0)
    return pl.pallas_call(
        functools.partial(hidden_kernel, block=block, tiles=tiles, rows=rows),
        grid_spec=pltpu.PrefetchScalarGridSpec(
            num_scalar_prefetch=1,
            grid=(2 * tiles,),
            in_specs=[
                pl.BlockSpec((tokens, block), lambda i, b: (0, jnp.minimum(i, tiles - 1))),
                pl.BlockSpec((tokens, block), lambda i, b: (0, jnp.maximum(i - tiles, 0))),
                pl.BlockSpec((block, width), lambda i, b: (place_of(b, i, tiles), 0)),
                pl.BlockSpec((8, tokens), whole),
                pl.BlockSpec((tokens, 1), whole),
            ],
            out_specs=[pl.BlockSpec((tokens, block), lambda i, b: (0, i))] + [pl.BlockSpec(shape, whole) for _ in range(2)],
            scratch_shapes=[pltpu.VMEM((tokens, width), f32), pltpu.VMEM((3, tokens, 1), f32)],
        ),
        out_shape=[jax.ShapeDtypeStruct((tokens, rows), bf16)] + [jax.ShapeDtypeStruct(shape, t) for t in (f32, f32)],
        compiler_params=params(46),
        cost_estimate=cost(2 * tokens * width * rows, 2 * width * rows),
    )(base, near, far, embedding, stats, target)


GROUP = 64


def embed_kernel(base, listed, bounds, grad, hid, cot_a, cot_b, ids, listed_col, *rest, block, scale, skip, steps, tiles):
    out, mixed = rest[-2:]
    out[...] = dot(grad[...], hid[...], 0, 0).astype(bf16)
    tile = place_of(base, skip + pl.program_id(0), tiles)
    split = cot_a.shape[0]

    opening = bounds[place_of(base, skip, tiles)]
    ending = bounds[place_of(base, skip + steps - 1, tiles) + 1]

    @pl.when(pl.program_id(0) == 0)
    def _():
        def group(g, carry):
            at = pl.multiple_of(g * GROUP, GROUP)
            hot = jnp.where(listed_col[pl.ds(opening + at, GROUP), :] == ids[...], 1.0, 0.0).astype(bf16)
            rows = dot(hot[:, :split], cot_a[...], 1, 0) + dot(hot[:, split:], cot_b[...], 1, 0)
            mixed[pl.ds(at, GROUP), :] = scale * rows
            return carry

        lax.fori_loop(0, (ending - opening + GROUP - 1) // GROUP, group, 0)

    def one(k, carry):
        row = listed[k] - tile * block
        start = pl.multiple_of((row // 16) * 16, 16)
        near_row = lax.broadcasted_iota(jnp.int32, (16, out.shape[1]), 0) == row - start
        add = jnp.where(near_row, mixed[pl.ds(k - opening, 1), :], 0.0)
        out[pl.ds(start, 16), :] = (out[pl.ds(start, 16), :].astype(f32) + add).astype(bf16)
        return carry

    lax.fori_loop(bounds[tile], bounds[tile + 1], one, 0)


def embed_grad(base, listed, bounds, grad, skip, steps, hid, cot, ids, column, block, scale, start):
    tokens, width = hid.shape
    rows = grad.shape[1]
    tiles = rows // block // 2
    whole = lambda i, *s: (0, 0)
    extra = [] if start is None else [start]
    return pl.pallas_call(
        functools.partial(embed_kernel, block=block, scale=scale, skip=skip, steps=steps, tiles=tiles),
        grid_spec=pltpu.PrefetchScalarGridSpec(
            num_scalar_prefetch=3,
            grid=(steps,),
            in_specs=[
                pl.BlockSpec((tokens, block), lambda i, *s: (0, skip + i)),
                pl.BlockSpec((tokens, width), whole),
                pl.BlockSpec((tokens // 2, width), whole),
                pl.BlockSpec((tokens // 2, width), whole),
                pl.BlockSpec((1, tokens), whole),
                pl.BlockSpec(column.shape, whole),
            ]
            + [pl.BlockSpec(memory_space=pl.ANY) for _ in extra],
            out_specs=pl.BlockSpec((block, width), lambda i, b, *s: (place_of(b, skip + i, tiles), 0)),
            scratch_shapes=[pltpu.VMEM((-(-tokens // GROUP) * GROUP, width), f32)],
        ),
        out_shape=jax.ShapeDtypeStruct((rows, width), bf16),
        input_output_aliases={9: 0} if extra else {},
        compiler_params=params(50),
        cost_estimate=cost(2 * tokens * width * block * steps, 2 * width * block * steps),
    )(base, listed, bounds, grad, hid, *cot, ids, column, *extra)


def flipped(x, span):
    lane = jnp.arange(x.shape[1], dtype=jnp.int32)
    return jnp.where((lane // span) % 2 == 0, jnp.roll(x, -span, 1), jnp.roll(x, span, 1))


def local_rows(ids, first_row, rows, block):
    at = ids - first_row
    count = at.shape[0]
    order = jnp.arange(count, dtype=jnp.int32)
    repeat = jnp.any((at[:, None] == at[None, :]) & (order[None, :] < order[:, None]), axis=1)
    lead = (at >= 0) & (at < rows) & ~repeat
    rank = jnp.sum((lead[None, :] & (at[None, :] < at[:, None])).astype(jnp.int32), axis=1)
    slots = jnp.arange(count + GROUP, dtype=jnp.int32)
    listed = jnp.sum(jnp.where(lead[None, :] & (rank[None, :] == slots[:, None]), at[None, :] + 1, 0), axis=1) - 1
    edges = block * jnp.arange(rows // block + 1, dtype=jnp.int32)
    bounds = jnp.sum((lead[None, :] & (at[None, :] < edges[:, None])).astype(jnp.int32), axis=1)
    return at[None, :], listed, listed[:, None], bounds


def permuted(hidden, embedding, embed_cotangent, input_ids, target_ids, tok_count, vocab_count):
    rows, width = embedding.shape
    own_tokens = hidden.shape[0]
    tokens = own_tokens * vocab_count
    half, half_rows = width // 2, rows // 2
    block = 1024
    bits = [vocab_count >> (k + 1) for k in range(vocab_count.bit_length() - 1)]
    core, place = lax.axis_index("tok"), lax.axis_index("vocab")
    base = jnp.stack([core, place]).astype(jnp.int32)
    across = functools.partial(swap, count=vocab_count)

    def grow(x, bit):
        return jnp.concatenate([x, across(x, bit)], axis=0)

    coded = jnp.stack(digits(target_ids) + digits(input_ids), axis=1)
    coded = jnp.pad(coded, ((0, 0), (0, 128 - coded.shape[1])))
    value = jnp.concatenate([hidden[:, :half], coded, hidden[:, half:]], axis=1)
    for bit in bits[:-2]:
        value = grow(value, bit)
    left = grow(value[:, : half + 128], bits[-2])
    right = grow(value[:, half + 128 :], bits[-1])
    left_other = across(left, bits[-1])
    right_other = across(right, bits[-2])

    cot = embed_cotangent
    for bit in bits[:-1]:
        other = across(cot, bit)
        cot = jnp.concatenate([cot, other], axis=0)

    sent, hid, target, inputs = first_logits(base, (left, left_other, right, right_other), embedding, half_rows, block)
    got = swap_tok(sent)
    ids, listed, column, bounds = local_rows(inputs[:, 0], place * rows, rows, block)
    target, ids, listed, column, bounds = lax.optimization_barrier((target, ids, listed, column, bounds))
    near, stats = own_logits(base, hid, embedding, got, target, block)
    far = swap_tok(near)

    stats = stats + swap_tok(stats)
    for k, bit in enumerate(bits):
        other = across(stats, bit)
        stats = stats + flipped(other, own_tokens << k)
    own_log = softcap + jnp.log(stats[0, :own_tokens])
    token_loss = own_log - softcap * stats[1, :own_tokens] + zloss_weight * own_log * own_log
    cot = (cot, across(tie(cot, stats), bits[-1]))

    grad, value, sent = hidden_sum(base, near, far, embedding, stats, target, 2 * block)

    def fold(keep, sent, bit):
        return keep + across(sent.astype(f16), bit).astype(f32)

    embed = functools.partial(
        embed_grad, hid=hid, cot=cot, ids=ids, column=column, block=block, scale=math.sqrt(width * tok_count)
    )
    tiles = half_rows // block
    embedding_grad = embed(base, listed, bounds, grad, 0, tiles, start=None)
    value = fold(value, sent, bits[-1])
    embedding_grad = embed(base, listed, bounds, grad, tiles, tiles // 2, start=embedding_grad)
    size = tokens // 4
    value = fold(value[:size], value[size:], bits[-2])
    embedding_grad = embed(
        base, listed, bounds, grad, tiles + tiles // 2, tiles - tiles // 2, start=embedding_grad
    )
    blocks = [value[k * own_tokens : (k + 1) * own_tokens] for k in range(4)]
    hidden_grad = blocks[0]
    for block_, bit in zip(blocks[1:], (bits[0], bits[1], bits[0] ^ bits[1])):
        hidden_grad = fold(hidden_grad, block_, bit)
    own = stats[:, :own_tokens]
    hidden_grad = (hidden_grad * sent_scale(own[0], own[1], own[2])[:, None]).astype(bf16)
    return (embedding_grad, hidden_grad, token_loss)


def solution(mesh):
    vocab_count, tok_count = mesh.shape["vocab"], mesh.shape["tok"]
    paired = tok_count == 2 and vocab_count == 16

    def local(hidden, embedding, embed_cotangent, input_ids, target_ids):
        rows, width = embedding.shape
        args = (hidden, embedding, embed_cotangent, input_ids, target_ids, tok_count)
        if not paired:
            return plain(*args)
        assert rows % 2048 == 0 and width % 256 == 0
        return permuted(*args, vocab_count)

    return jax.shard_map(
        local,
        mesh=mesh,
        in_specs=(P("vocab", "tok"), P("vocab", "tok"), P("vocab", "tok"), P("vocab"), P("vocab")),
        out_specs=(P("vocab", "tok"), P("vocab", "tok"), P("vocab")),
        check_vma=False,
    )
```
